32 devices in a mesh: grp: 2 (over y), col: 4 (over z), blk: 4 (over x, core).
Axes of the slice: x: 2, y: 2, z: 4, core: 2. Of those that a mesh axis runs over, the one named last changes fastest.
Arguments:
- boundary: bfloat16 [32, 192, 576], P(('grp', 'col'), 'blk'), parts along dimension 0, may hold values from -6 to 6
- row_tensor: bfloat16 [32, 6, 6, 6, 6], P(('grp', 'col')), parts along dimension 0, may hold values from -1.5 to 1.5
- left_proj: bfloat16 [32, 192, 576], P(('grp', 'col'), 'blk'), parts along dimension 0, may hold values from -0.75 to 0.75
- right_proj: bfloat16 [32, 192, 576], P(('grp', 'col'), 'blk'), parts along dimension 0, may hold values from -0.3125 to 0.3125
- leg_parity: int32 [32, 3, 6], P('grp'), parts along dimension 0, may hold values from 0 to 1
- bond_charges: int32 [32, 2], P('grp'), parts along dimension 0, may hold values from 32 to 96, as said below
Outputs:
- new_boundary: bfloat16 [32, 192, 576], P(('grp', 'col'), 'blk'), parts along dimension 0
The draws below stay inside these ranges and needn't reach their ends.
There are 2 independent parts, one for each index of `grp`. The reference program is written for one: setup_inputs(seed, part) draws one part's arguments, and reference() takes and returns one part's arrays. A program takes and returns all parts, laid end to end along the dimension named above; each array names one. Nothing has to cross between parts.
Inputs may be any that keep to these rules, and one draw needn't show every extreme that they name: `bond_charges`: odd counts are 128 minus these, so neither block of a bond holds more than 96 live rows; some bond has an even count of 96 and some bond an odd count of 96. `leg_parity`: [c, 0] is the horizontal leg left of column c, [c, 1] the vertical leg between boundary and row, [c, 2] the outgoing vertical leg.
All inputs are finite; a program needn't handle non-finite values.
Results may differ from the reference program's by a relative error of at most 0.0057.
Values may be sent and summed in bfloat16 or wider, within the bound.
A program may use at most 64 MiB of HBM per device.

```python
import jax
import jax.numpy as jnp
from jax import lax

CHI = 128
BLOCK = 96
D = 6
COLS = 16
PAD = 192


def draw_bond_charges(key, part):
    first_key, second_key, third_key = jax.random.split(jax.random.fold_in(key, 17), 3)
    counts = jax.random.randint(first_key, (COLS, 2), CHI - BLOCK, BLOCK + 1, dtype=jnp.int32)
    even_full = jax.random.randint(second_key, (), 0, COLS, dtype=jnp.int32)
    odd_full = jax.random.randint(third_key, (), 0, COLS, dtype=jnp.int32)
    counts = counts.at[even_full, 0].set(BLOCK)
    counts = counts.at[odd_full, 1].set(CHI - BLOCK)
    return counts


def plant(drawn, stream_key, least, largest):
    spot = [jax.random.randint(jax.random.fold_in(stream_key, axis), (), 0, length) for axis, length in enumerate(drawn.shape)]
    longest = drawn.shape.index(max(drawn.shape))
    neighbour = spot[:longest] + [(spot[longest] + 1) % drawn.shape[longest]] + spot[longest + 1:]
    return drawn.at[tuple(spot)].set(least).at[tuple(neighbour)].set(largest)


def level_of(key, extent, cuts, least, top_value):
    def one(axis_at, parts):
        heights = jax.random.uniform(jax.random.fold_in(jax.random.fold_in(key, 6), axis_at), (parts,), jnp.float32, least / len(cuts), top_value / len(cuts))
        return jnp.repeat(jnp.exp(heights), extent[axis_at] // parts).reshape((-1,) + (1,) * (len(extent) - axis_at - 1))

    loudness = one(*cuts[0])
    for cut in cuts[1:]:
        loudness = loudness * one(*cut)
    return loudness


def bell_draw(key, shape, spread, reach, pieces=(), kind=jnp.bfloat16):
    drawn = spread * jax.random.normal(key, shape, jnp.float32)
    if pieces:
        drawn = drawn * level_of(key, shape, pieces, -0.22, 0.18)
    return jnp.clip(drawn, -reach, reach).astype(kind)


def setup_inputs(seed: int = 0, part: int = 0) -> dict:
    arg_keys = jax.random.split(jax.random.key(seed), 7)
    part_keys = jax.random.split(jax.random.fold_in(arg_keys[6], part), 7)
    return {
        "boundary": bell_draw(part_keys[0], (COLS, PAD, D * BLOCK), 1.0, 6.0, ((0, 4), (1, 4))),
        "row_tensor": bell_draw(part_keys[1], (COLS, D, D, D, D), (D * D // 2) ** -0.5, 1.5, ((0, 4),)),
        "left_proj": bell_draw(part_keys[2], (COLS, PAD, D * BLOCK), (CHI // 2) ** -0.5, 0.75, ((0, 4), (1, 4))),
        "right_proj": bell_draw(part_keys[3], (COLS, PAD, D * BLOCK), (D * CHI // 2) ** -0.5, 0.3125, ((0, 4), (1, 4))),
        "leg_parity": plant(jax.random.randint(part_keys[4], (COLS, 3, D), 0, 2), jax.random.fold_in(part_keys[4], 1), 0, 1).astype(jnp.int32),
        "bond_charges": draw_bond_charges(jax.random.fold_in(jax.random.fold_in(arg_keys[6], part), 71), part),
    }


def live_rows(count, parity, position):
    limit = jnp.where(parity == 0, count, CHI - count)
    return (position < limit).astype(jnp.float32)


def reference(boundary, row_tensor, left_proj, right_proj, leg_parity, bond_charges):
    padded = 2 * BLOCK
    bound_all = boundary.reshape(COLS, padded, D, BLOCK)
    left_all = left_proj.reshape(COLS, padded, D, BLOCK)
    right_all = jnp.roll(right_proj.reshape(COLS, padded, D, BLOCK), -1, axis=0)
    charges_next = jnp.roll(bond_charges, -1, axis=0)
    legs_next = jnp.roll(leg_parity, -1, axis=0)
    indices = jnp.arange(padded, dtype=jnp.int32)
    parity_idx = indices // BLOCK
    position = indices % BLOCK
    inside = jnp.arange(BLOCK, dtype=jnp.int32)

    def column_step(inputs):
        bound_col, row_col, left_col, right_col, charge_here, charge_next, leg_here, leg_next = inputs
        left_leg = leg_here[0]
        up_leg = leg_here[1]
        down_leg = leg_here[2]
        right_leg = leg_next[0]
        bound_sel = (parity_idx[:, None] + up_leg[None, :]) % 2
        bound_mask = live_rows(charge_here[0], parity_idx, position)[:, None, None] * live_rows(
            charge_next[0], bound_sel[:, :, None], inside[None, None, :])
        bound_m = bound_col * bound_mask.astype(jnp.bfloat16)
        left_sel = (parity_idx[:, None] + left_leg[None, :]) % 2
        left_mask = live_rows(charge_here[1], parity_idx, position)[:, None, None] * live_rows(
            charge_here[0], left_sel[:, :, None], inside[None, None, :])
        left_m = left_col * left_mask.astype(jnp.bfloat16)
        left_dense = jnp.concatenate([
            left_m * (left_sel == 0).astype(jnp.bfloat16)[:, :, None],
            left_m * (left_sel == 1).astype(jnp.bfloat16)[:, :, None]], axis=2)
        right_sel = (parity_idx[:, None] + right_leg[None, :]) % 2
        right_mask = live_rows(charge_next[0], parity_idx, position)[:, None, None] * live_rows(
            charge_next[1], right_sel[:, :, None], inside[None, None, :])
        right_m = right_col * right_mask.astype(jnp.bfloat16)
        row_mask = ((left_leg[:, None, None, None] + up_leg[None, :, None, None]
                     + down_leg[None, None, :, None] + right_leg[None, None, None, :]) % 2 == 0).astype(jnp.float32)
        row_mask = row_mask * (1 - 2 * left_leg[:, None, None, None] * up_leg[None, :, None, None]).astype(jnp.float32)
        row_m = row_col * row_mask.astype(jnp.bfloat16)
        absorbed = jnp.dot(left_dense.reshape(padded * D, padded), bound_m.reshape(padded, D * BLOCK),
                           preferred_element_type=jnp.float32)
        absorbed = absorbed.astype(jnp.bfloat16).reshape(padded, D, D, BLOCK)
        mixed = jnp.einsum("plub,ludr->pdrb", absorbed.astype(jnp.float32), row_m.astype(jnp.float32))
        block_par = (parity_idx[:, None, None] + down_leg[None, :, None] + right_leg[None, None, :]) % 2
        sign_flip = (1 - 2 * block_par * down_leg[None, :, None]).astype(jnp.float32)
        mixed = (mixed * sign_flip[:, :, :, None]).astype(jnp.bfloat16)
        mixed_dense = jnp.concatenate([
            mixed * (block_par == 0).astype(jnp.bfloat16)[:, :, :, None],
            mixed * (block_par == 1).astype(jnp.bfloat16)[:, :, :, None]], axis=3)
        right_rb = jnp.transpose(right_m, (1, 0, 2)).reshape(D * padded, BLOCK)
        result = jnp.dot(mixed_dense.reshape(padded * D, D * padded), right_rb,
                         preferred_element_type=jnp.float32)
        return result.astype(jnp.bfloat16).reshape(padded, D * BLOCK)

    return lax.map(column_step, (bound_all, row_tensor, left_all, right_all,
                                 bond_charges, charges_next, leg_parity, legs_next))
```

```python
import functools

import jax
import jax.numpy as jnp
from jax import lax
from jax.experimental import pallas as pl
from jax.experimental.pallas import tpu as pltpu
from jax.sharding import PartitionSpec as P

CHI = 128
BLOCK = 96
D = 6
LANES = 128
SUB = 8
KRON = D * D * SUB
MESH = pl.DeviceIdType.MESH


def limit_of(count, parity):
    return jnp.where(parity == 0, count, CHI - count)


def pick(index, scalars):
    acc = jnp.zeros(index.shape, jnp.int32)
    for at, value in enumerate(scalars):
        acc = jnp.where(index == at, value, acc)
    return acc


def kernel(
    cols, subs, n_blk, n_col,
    bound_hbm, row_hbm, left_hbm, right_hbm, legs, charges, out_ref,
    bound_all, right_all, left_own, row_own, left_dense, kron, bound_pad, right_pad,
    local_sem, send_sem, recv_sem, z_sem,
):
    me = lax.axis_index("blk")
    here = lax.axis_index("col")
    partner = me + 1 - 2 * (me % 2)
    across = (me + 2) % n_blk
    across_partner = (partner + 2) % n_blk
    col_left = (here + n_col - 1) % n_col
    col_right = (here + 1) % n_col
    all_cols = cols * n_col
    parity = me // 2
    row_base = (me % 2) * subs

    own_copies = [
        pltpu.make_async_copy(bound_hbm, bound_all.at[me], local_sem.at[0]),
        pltpu.make_async_copy(
            right_hbm.at[pl.ds(1, cols - 1)], right_all.at[me, pl.ds(0, cols - 1)], local_sem.at[1]
        ),
        pltpu.make_async_copy(left_hbm, left_own, local_sem.at[2]),
        pltpu.make_async_copy(row_hbm, row_own, local_sem.at[3]),
    ]
    for copy in own_copies:
        copy.start()

    barrier = pltpu.get_barrier_semaphore()
    for target in ({"blk": partner}, {"blk": across}, {"col": col_left}, {"col": col_right}):
        pl.semaphore_signal(barrier, inc=1, device_id=target, device_id_type=MESH)
    pl.semaphore_wait(barrier, 4)

    def z_copy():
        return pltpu.make_async_remote_copy(
            src_ref=right_hbm.at[0], dst_ref=right_all.at[me, cols - 1],
            send_sem=z_sem.at[0], recv_sem=z_sem.at[1],
            device_id={"col": col_left}, device_id_type=MESH,
        )

    def link(which, route, c):
        buffer = bound_all if which == 0 else right_all
        slot = across if route == 2 else me
        target = across if route == 0 else partner
        return pltpu.make_async_remote_copy(
            src_ref=buffer.at[slot, c], dst_ref=buffer.at[slot, c],
            send_sem=send_sem.at[which, route, c], recv_sem=recv_sem.at[which, route, c],
            device_id={"blk": target}, device_id_type=MESH,
        )

    z_copy().start()
    own_copies[0].wait()
    link(0, 0, 0).start()
    own_copies[1].wait()
    for c in range(cols):
        if c > 0:
            link(0, 0, c).start()
        if c < cols - 1:
            link(1, 0, c).start()
    for c in range(cols):
        link(0, 1, c).start()
        if c < cols - 1:
            link(1, 1, c).start()
    own_copies[2].wait()
    own_copies[3].wait()

    bound_pad[...] = jnp.zeros_like(bound_pad)
    right_pad[...] = jnp.zeros_like(right_pad)
    left_dense[...] = jnp.zeros_like(left_dense)

    z_copy().wait_recv()
    link(1, 0, cols - 1).start()
    link(1, 1, cols - 1).start()

    def scalars(c):
        at = here * cols + c
        nxt = (at + 1) % all_cols
        p0 = [legs[at, 0, k] for k in range(D)]
        p1 = [legs[at, 1, k] for k in range(D)]
        p2 = [legs[at, 2, k] for k in range(D)]
        pr = [legs[nxt, 0, k] for k in range(D)]
        return p0, p1, p2, pr, charges[at, 0], charges[at, 1], charges[nxt, 0], charges[nxt, 1]

    lane96 = lax.broadcasted_iota(jnp.int32, (subs, BLOCK), 1)
    row96 = lax.broadcasted_iota(jnp.int32, (subs, BLOCK), 0)

    def as_mask(condition):
        return jnp.where(condition, 1.0, 0.0)

    def prepare(c, _):
        p0, p1, p2, pr, in_here, out_here, in_next, out_next = scalars(c)
        for l in range(D):
            q = (parity + p0[l]) % 2
            segment = left_own[c, :, l * BLOCK:(l + 1) * BLOCK]
            keep = lane96 < limit_of(in_here, q)
            even = as_mask(keep & (q == 0)).astype(jnp.bfloat16)
            odd = as_mask(keep & (q == 1)).astype(jnp.bfloat16)
            left_dense[c, l * subs:(l + 1) * subs, 0:BLOCK] = segment * even
            left_dense[c, l * subs:(l + 1) * subs, LANES:LANES + BLOCK] = segment * odd
        w = row_own[c].astype(jnp.float32).reshape(D * D, D, D)
        w = jnp.concatenate([w, jnp.zeros((D * D, SUB - D, D), jnp.float32)], axis=1)
        w = w.reshape(KRON, D).astype(jnp.bfloat16)
        spread_row = lax.broadcasted_iota(jnp.int32, (KRON, D), 0)
        spread_lane = lax.broadcasted_iota(jnp.int32, (KRON, D), 1)
        spread = as_mask((spread_row // SUB) % D == spread_lane).astype(jnp.bfloat16)
        big = lax.dot_general(
            spread, w, (((1,), (1,)), ((), ())), preferred_element_type=jnp.float32
        )
        row = lax.broadcasted_iota(jnp.int32, (KRON, KRON), 0)
        lane = lax.broadcasted_iota(jnp.int32, (KRON, KRON), 1)
        big = jnp.where(row // (D * SUB) == lane % SUB, big, 0.0).astype(jnp.bfloat16)
        group = as_mask(row // SUB == lane // SUB).astype(jnp.bfloat16)
        big = jnp.dot(big, group, preferred_element_type=jnp.float32)
        rows = lax.broadcasted_iota(jnp.int32, (KRON, 1), 0)
        lanes = lax.broadcasted_iota(jnp.int32, (1, KRON), 1)
        down = pick(rows // (D * SUB), p2)
        right = pick((rows // SUB) % D, pr)
        left = pick(lanes // (D * SUB), p0)
        up = pick((lanes // SUB) % D, p1)
        row_sign = 1 - 2 * (((parity + down + right) % 2) * down)
        lane_sign = 1 - 2 * left * up
        row_par = (down + right) % 2
        lane_par = (left + up) % 2
        same = row_par * lane_par + (1 - row_par) * (1 - lane_par)
        factor = (same * row_sign * lane_sign).astype(jnp.float32)
        kron[c] = jnp.where(row % SUB == lane % SUB, big * factor, 0.0).astype(jnp.bfloat16)
        return _

    lax.fori_loop(0, cols, prepare, 0)

    def column(c, _):
        p0, p1, p2, pr, in_here, out_here, in_next, out_next = scalars(c)
        link(0, 0, c).wait_recv()
        link(0, 2, c).start()
        link(0, 1, c).wait_recv()
        link(0, 2, c).wait_recv()
        for slot in range(n_blk):
            top = (slot // 2) * LANES + (slot % 2) * subs
            for u in range(D):
                bound_pad[top:top + subs, u * LANES:u * LANES + BLOCK] = bound_all[
                    slot, c, :, u * BLOCK:(u + 1) * BLOCK
                ]
        absorbed = jnp.dot(left_dense[c], bound_pad[...], preferred_element_type=jnp.float32)
        high = subs // SUB
        x = jnp.concatenate(
            [
                jnp.concatenate(
                    [
                        absorbed[l * subs + h * SUB:l * subs + (h + 1) * SUB, u * LANES:(u + 1) * LANES]
                        for h in range(high)
                    ],
                    axis=1,
                )
                for l in range(D)
                for u in range(D)
            ],
            axis=0,
        ).astype(jnp.bfloat16)
        mixed = jnp.dot(kron[c], x, preferred_element_type=jnp.float32)
        y = jnp.concatenate(
            [
                jnp.concatenate(
                    [
                        mixed[(d * D + r) * SUB:(d * D + r + 1) * SUB, h * LANES:(h + 1) * LANES]
                        for r in range(D)
                    ],
                    axis=1,
                )
                for d in range(D)
                for h in range(high)
            ],
            axis=0,
        ).astype(jnp.bfloat16)

        link(1, 0, c).wait_recv()
        link(1, 2, c).start()
        link(1, 1, c).wait_recv()
        link(1, 2, c).wait_recv()
        for half in range(2):
            even_live = as_mask(row96 + half * subs < in_next).astype(jnp.bfloat16)
            odd_live = as_mask(row96 + half * subs < CHI - in_next).astype(jnp.bfloat16)
            for r in range(D):
                span = slice(r * BLOCK, (r + 1) * BLOCK)
                even = right_all[half, c, :, span] * even_live
                odd = right_all[2 + half, c, :, span] * odd_live
                straight = (parity + pr[r]) % 2 == 0
                top = r * LANES + half * subs
                right_pad[top:top + subs, 0:BLOCK] = jnp.where(straight, even, odd)
                right_pad[top:top + subs, LANES:LANES + BLOCK] = jnp.where(straight, odd, even)
        result = jnp.dot(y, right_pad[...], preferred_element_type=jnp.float32)
        row_live = row96 + row_base < limit_of(out_here, parity)
        for d in range(D):
            rows = slice(d * subs, (d + 1) * subs)
            part = jnp.where(p2[d] == 0, result[rows, 0:BLOCK], result[rows, LANES:LANES + BLOCK])
            live = row_live & (lane96 < limit_of(out_next, (parity + p2[d]) % 2))
            out_ref[c, :, d * BLOCK:(d + 1) * BLOCK] = jnp.where(live, part, 0.0).astype(jnp.bfloat16)
        return _

    lax.fori_loop(0, cols, column, 0)

    z_copy().wait_send()
    for c in range(cols):
        for which in range(2):
            for route in range(3):
                link(which, route, c).wait_send()


def per_device(n_blk, n_col, boundary, row_tensor, left_proj, right_proj, leg_parity, bond_charges):
    cols, subs, merged = boundary.shape
    bf16 = jnp.bfloat16
    hbm = pl.BlockSpec(memory_space=pl.ANY)
    smem = pl.BlockSpec(memory_space=pltpu.SMEM)
    return pl.pallas_call(
        functools.partial(kernel, cols, subs, n_blk, n_col),
        out_shape=jax.ShapeDtypeStruct(boundary.shape, bf16),
        in_specs=[hbm, hbm, hbm, hbm, smem, smem],
        out_specs=pl.BlockSpec(memory_space=pltpu.VMEM),
        scratch_shapes=[
            pltpu.VMEM((n_blk, cols, subs, merged), bf16),
            pltpu.VMEM((n_blk, cols, subs, merged), bf16),
            pltpu.VMEM((cols, subs, merged), bf16),
            pltpu.VMEM(row_tensor.shape, bf16),
            pltpu.VMEM((cols, D * subs, 2 * LANES), bf16),
            pltpu.VMEM((cols, KRON, KRON), bf16),
            pltpu.VMEM((2 * LANES, D * LANES), bf16),
            pltpu.VMEM((D * LANES, 2 * LANES), bf16),
            pltpu.SemaphoreType.DMA((4,)),
            pltpu.SemaphoreType.DMA((2, 3, cols)),
            pltpu.SemaphoreType.DMA((2, 3, cols)),
            pltpu.SemaphoreType.DMA((2,)),
        ],
        compiler_params=pltpu.CompilerParams(
            collective_id=0, has_side_effects=True, vmem_limit_bytes=48 * 1024 * 1024
        ),
    )(boundary, row_tensor, left_proj, right_proj, leg_parity, bond_charges)


def solution(mesh):
    in_specs = (
        P(("grp", "col"), "blk", None),
        P(("grp", "col"), None, None, None, None),
        P(("grp", "col"), "blk", None),
        P(("grp", "col"), "blk", None),
        P("grp", None, None),
        P("grp", None),
    )
    out_specs = P(("grp", "col"), "blk", None)
    body = functools.partial(per_device, mesh.shape["blk"], mesh.shape["col"])
    return jax.shard_map(body, mesh=mesh, in_specs=in_specs, out_specs=out_specs, check_vma=False)
```

```python
import functools

import jax
import jax.numpy as jnp
from jax import lax
from jax.experimental import pallas as pl
from jax.experimental.pallas import tpu as pltpu
from jax.sharding import PartitionSpec as P

CHI = 128
BLOCK = 96
D = 6
LANES = 128
SUB = 8
KRON = D * D * SUB
MESH = pl.DeviceIdType.MESH


def limit_of(count, parity):
    return jnp.where(parity == 0, count, CHI - count)


def pick(index, scalars):
    acc = jnp.zeros(index.shape, jnp.int32)
    for at, value in enumerate(scalars):
        acc = jnp.where(index == at, value, acc)
    return acc


def kernel(
    cols, subs, n_blk, n_col,
    bound_hbm, row_hbm, left_hbm, right_hbm, legs, charges, out_ref,
    bound_all, right_all, left_own, row_own, row_wide, left_dense, kron, bound_pad, right_pad,
    local_sem, send_sem, recv_sem, z_sem,
):
    me = lax.axis_index("blk")
    here = lax.axis_index("col")
    partner = me + 1 - 2 * (me % 2)
    across = (me + 2) % n_blk
    across_partner = (partner + 2) % n_blk
    col_left = (here + n_col - 1) % n_col
    col_right = (here + 1) % n_col
    all_cols = cols * n_col
    parity = me // 2
    row_base = (me % 2) * subs

    own_copies = [
        pltpu.make_async_copy(bound_hbm, bound_all.at[me], local_sem.at[0]),
        pltpu.make_async_copy(
            right_hbm.at[pl.ds(1, cols - 1)], right_all.at[me, pl.ds(0, cols - 1)], local_sem.at[1]
        ),
        pltpu.make_async_copy(left_hbm, left_own, local_sem.at[2]),
        pltpu.make_async_copy(row_hbm, row_own, local_sem.at[3]),
    ]
    for copy in own_copies:
        copy.start()

    barrier = pltpu.get_barrier_semaphore()
    for target in ({"blk": partner}, {"blk": across}, {"col": col_left}, {"col": col_right}):
        pl.semaphore_signal(barrier, inc=1, device_id=target, device_id_type=MESH)
    pl.semaphore_wait(barrier, 4)

    def z_copy():
        return pltpu.make_async_remote_copy(
            src_ref=right_hbm.at[0], dst_ref=right_all.at[me, cols - 1],
            send_sem=z_sem.at[0], recv_sem=z_sem.at[1],
            device_id={"col": col_left}, device_id_type=MESH,
        )

    def link(which, route, c):
        buffer = bound_all if which == 0 else right_all
        slot = across if route == 2 else me
        target = across if route == 0 else partner
        return pltpu.make_async_remote_copy(
            src_ref=buffer.at[slot, c], dst_ref=buffer.at[slot, c],
            send_sem=send_sem.at[which, route, c], recv_sem=recv_sem.at[which, route, c],
            device_id={"blk": target}, device_id_type=MESH,
        )

    z_copy().start()
    own_copies[0].wait()
    link(0, 0, 0).start()
    own_copies[1].wait()
    for c in range(cols):
        if c > 0:
            link(0, 0, c).start()
        if c < cols - 1:
            link(1, 0, c).start()
    for c in range(cols):
        link(0, 1, c).start()
        if c < cols - 1:
            link(1, 1, c).start()
    own_copies[2].wait()
    own_copies[3].wait()

    bound_pad[...] = jnp.zeros_like(bound_pad)
    right_pad[...] = jnp.zeros_like(right_pad)
    left_dense[...] = jnp.zeros_like(left_dense)

    z_copy().wait_recv()
    link(1, 0, cols - 1).start()
    link(1, 1, cols - 1).start()

    def scalars(c):
        at = here * cols + c
        nxt = (at + 1) % all_cols
        p0 = [legs[0, k, at] for k in range(D)]
        p1 = [legs[1, k, at] for k in range(D)]
        p2 = [legs[2, k, at] for k in range(D)]
        pr = [legs[0, k, nxt] for k in range(D)]
        return p0, p1, p2, pr, charges[0, at], charges[1, at], charges[0, nxt], charges[1, nxt]

    lane96 = lax.broadcasted_iota(jnp.int32, (subs, BLOCK), 1)
    row96 = lax.broadcasted_iota(jnp.int32, (subs, BLOCK), 0)

    def as_mask(condition):
        return jnp.where(condition, 1.0, 0.0)

    def prepare(c, _):
        p0, p1, p2, pr, in_here, out_here, in_next, out_next = scalars(c)
        for l in range(D):
            q = (parity + p0[l]) % 2
            segment = left_own[c, :, l * BLOCK:(l + 1) * BLOCK]
            keep = lane96 < limit_of(in_here, q)
            even = as_mask(keep & (q == 0)).astype(jnp.bfloat16)
            odd = as_mask(keep & (q == 1)).astype(jnp.bfloat16)
            left_dense[c, l * subs:(l + 1) * subs, 0:BLOCK] = segment * even
            left_dense[c, l * subs:(l + 1) * subs, LANES:LANES + BLOCK] = segment * odd
        w = row_wide[pl.ds(c, D * D * D, stride=cols), :][:, 0:D].astype(jnp.bfloat16)
        spread_row = lax.broadcasted_iota(jnp.int32, (KRON, D), 0)
        spread_lane = lax.broadcasted_iota(jnp.int32, (KRON, D), 1)
        spread = as_mask((spread_row // SUB) % D == spread_lane).astype(jnp.bfloat16)
        big = lax.dot_general(
            spread, w, (((1,), (1,)), ((), ())), preferred_element_type=jnp.float32
        )
        row = lax.broadcasted_iota(jnp.int32, (KRON, KRON), 0)
        lane = lax.broadcasted_iota(jnp.int32, (KRON, KRON), 1)
        flat_row = lax.broadcasted_iota(jnp.int32, (KRON, D * D * D), 0)
        flat_lane = lax.broadcasted_iota(jnp.int32, (KRON, D * D * D), 1)
        big = jnp.where(flat_row // (D * SUB) == flat_lane % D, big, 0.0).astype(jnp.bfloat16)
        group_row = lax.broadcasted_iota(jnp.int32, (D * D * D, KRON), 0)
        group_lane = lax.broadcasted_iota(jnp.int32, (D * D * D, KRON), 1)
        group = as_mask(group_row // D == group_lane // SUB).astype(jnp.bfloat16)
        big = jnp.dot(big, group, preferred_element_type=jnp.float32)
        rows = lax.broadcasted_iota(jnp.int32, (KRON, 1), 0)
        lanes = lax.broadcasted_iota(jnp.int32, (1, KRON), 1)
        down = pick(rows // (D * SUB), p2)
        right = pick((rows // SUB) % D, pr)
        left = pick(lanes // (D * SUB), p0)
        up = pick((lanes // SUB) % D, p1)
        row_sign = 1 - 2 * (((parity + down + right) % 2) * down)
        lane_sign = 1 - 2 * left * up
        row_par = (down + right) % 2
        lane_par = (left + up) % 2
        same = row_par * lane_par + (1 - row_par) * (1 - lane_par)
        factor = (same * row_sign * lane_sign).astype(jnp.float32)
        kron[c] = jnp.where(row % SUB == lane % SUB, big * factor, 0.0).astype(jnp.bfloat16)
        return _

    row_wide[:, 0:D] = row_own[...].astype(jnp.float32)
    lax.fori_loop(0, cols, prepare, 0)

    def column(c, _):
        p0, p1, p2, pr, in_here, out_here, in_next, out_next = scalars(c)
        link(0, 0, c).wait_recv()
        link(0, 2, c).start()
        link(0, 1, c).wait_recv()
        link(0, 2, c).wait_recv()
        for slot in range(n_blk):
            top = (slot // 2) * LANES + (slot % 2) * subs
            for u in range(D):
                bound_pad[top:top + subs, u * LANES:u * LANES + BLOCK] = bound_all[
                    slot, c, :, u * BLOCK:(u + 1) * BLOCK
                ]
        absorbed = jnp.dot(left_dense[c], bound_pad[...], preferred_element_type=jnp.float32)
        high = subs // SUB
        x = jnp.concatenate(
            [
                jnp.concatenate(
                    [
                        absorbed[l * subs + h * SUB:l * subs + (h + 1) * SUB, u * LANES:(u + 1) * LANES]
                        for h in range(high)
                    ],
                    axis=1,
                )
                for l in range(D)
                for u in range(D)
            ],
            axis=0,
        ).astype(jnp.bfloat16)
        mixed = jnp.dot(kron[c], x, preferred_element_type=jnp.float32)
        y = jnp.concatenate(
            [
                jnp.concatenate(
                    [
                        mixed[(d * D + r) * SUB:(d * D + r + 1) * SUB, h * LANES:(h + 1) * LANES]
                        for r in range(D)
                    ],
                    axis=1,
                )
                for d in range(D)
                for h in range(high)
            ],
            axis=0,
        ).astype(jnp.bfloat16)

        link(1, 0, c).wait_recv()
        link(1, 2, c).start()
        link(1, 1, c).wait_recv()
        link(1, 2, c).wait_recv()
        for half in range(2):
            even_live = as_mask(row96 + half * subs < in_next).astype(jnp.bfloat16)
            odd_live = as_mask(row96 + half * subs < CHI - in_next).astype(jnp.bfloat16)
            for r in range(D):
                span = slice(r * BLOCK, (r + 1) * BLOCK)
                even = right_all[half, c, :, span] * even_live
                odd = right_all[2 + half, c, :, span] * odd_live
                straight = (parity + pr[r]) % 2 == 0
                top = r * LANES + half * subs
                right_pad[top:top + subs, 0:BLOCK] = jnp.where(straight, even, odd)
                right_pad[top:top + subs, LANES:LANES + BLOCK] = jnp.where(straight, odd, even)
        result = jnp.dot(y, right_pad[...], preferred_element_type=jnp.float32)
        row_live = row96 + row_base < limit_of(out_here, parity)
        for d in range(D):
            rows = slice(d * subs, (d + 1) * subs)
            part = jnp.where(p2[d] == 0, result[rows, 0:BLOCK], result[rows, LANES:LANES + BLOCK])
            live = row_live & (lane96 < limit_of(out_next, (parity + p2[d]) % 2))
            out_ref[c, :, d * BLOCK:(d + 1) * BLOCK] = jnp.where(live, part, 0.0).astype(jnp.bfloat16)
        return _

    lax.fori_loop(0, cols, column, 0)

    z_copy().wait_send()
    for c in range(cols):
        for which in range(2):
            for route in range(3):
                link(which, route, c).wait_send()


def per_device(n_blk, n_col, boundary, row_tensor, left_proj, right_proj, leg_parity, bond_charges):
    cols, subs, merged = boundary.shape
    bf16 = jnp.bfloat16
    row_flat = row_tensor.transpose(1, 2, 3, 0, 4).reshape(D * D * D * cols, D)
    hbm = pl.BlockSpec(memory_space=pl.ANY)
    smem = pl.BlockSpec(memory_space=pltpu.SMEM)
    return pl.pallas_call(
        functools.partial(kernel, cols, subs, n_blk, n_col),
        out_shape=jax.ShapeDtypeStruct(boundary.shape, bf16),
        in_specs=[hbm, hbm, hbm, hbm, smem, smem],
        out_specs=pl.BlockSpec(memory_space=pltpu.VMEM),
        scratch_shapes=[
            pltpu.VMEM((n_blk, cols, subs, merged), bf16),
            pltpu.VMEM((n_blk, cols, subs, merged), bf16),
            pltpu.VMEM((cols, subs, merged), bf16),
            pltpu.VMEM(row_flat.shape, bf16),
            pltpu.VMEM((row_flat.shape[0], LANES), jnp.float32),
            pltpu.VMEM((cols, D * subs, 2 * LANES), bf16),
            pltpu.VMEM((cols, KRON, KRON), bf16),
            pltpu.VMEM((2 * LANES, D * LANES), bf16),
            pltpu.VMEM((D * LANES, 2 * LANES), bf16),
            pltpu.SemaphoreType.DMA((4,)),
            pltpu.SemaphoreType.DMA((2, 3, cols)),
            pltpu.SemaphoreType.DMA((2, 3, cols)),
            pltpu.SemaphoreType.DMA((2,)),
        ],
        compiler_params=pltpu.CompilerParams(
            collective_id=0, has_side_effects=True
        ),
    )(boundary, row_flat, left_proj, right_proj, leg_parity.transpose(1, 2, 0), bond_charges.T)


def solution(mesh):
    in_specs = (
        P(("grp", "col"), "blk", None),
        P(("grp", "col"), None, None, None, None),
        P(("grp", "col"), "blk", None),
        P(("grp", "col"), "blk", None),
        P("grp", None, None),
        P("grp", None),
    )
    out_specs = P(("grp", "col"), "blk", None)
    body = functools.partial(per_device, mesh.shape["blk"], mesh.shape["col"])
    return jax.shard_map(body, mesh=mesh, in_specs=in_specs, out_specs=out_specs, check_vma=False)
```

```python
import functools

import jax
import jax.numpy as jnp
from jax import lax
from jax.experimental import pallas as pl
from jax.experimental.pallas import tpu as pltpu
from jax.sharding import PartitionSpec as P

CHI = 128
BLOCK = 96
D = 6
LANES = 128
SUB = 8
KRON = D * D * SUB
MESH = pl.DeviceIdType.MESH


def limit_of(count, parity):
    return jnp.where(parity == 0, count, CHI - count)


def pick(index, scalars):
    acc = jnp.zeros(index.shape, jnp.int32)
    for at, value in enumerate(scalars):
        acc = jnp.where(index == at, value, acc)
    return acc


def kernel(
    cols, subs, n_blk, n_col,
    bound_hbm, row_hbm, left_hbm, right_hbm, legs, charges, out_ref,
    bound_all, right_all, left_own, row_own, row_wide, left_dense, kron, bound_pad, right_pad, y_ref, out_own,
    local_sem, send_sem, recv_sem, z_sem, out_sem,
):
    me = lax.axis_index("blk")
    here = lax.axis_index("col")
    partner = me + 1 - 2 * (me % 2)
    across = (me + 2) % n_blk
    across_partner = (partner + 2) % n_blk
    col_left = (here + n_col - 1) % n_col
    col_right = (here + 1) % n_col
    all_cols = cols * n_col
    parity = me // 2
    row_base = (me % 2) * subs

    own_copies = [
        pltpu.make_async_copy(bound_hbm, bound_all.at[me], local_sem.at[0]),
        pltpu.make_async_copy(
            right_hbm.at[pl.ds(1, cols - 1)], right_all.at[me, pl.ds(0, cols - 1)], local_sem.at[1]
        ),
        pltpu.make_async_copy(left_hbm, left_own, local_sem.at[2]),
        pltpu.make_async_copy(row_hbm, row_own, local_sem.at[3]),
    ]
    for copy in own_copies:
        copy.start()

    barrier = pltpu.get_barrier_semaphore()
    for target in ({"blk": partner}, {"blk": across}, {"col": col_left}, {"col": col_right}):
        pl.semaphore_signal(barrier, inc=1, device_id=target, device_id_type=MESH)
    bound_pad[...] = jnp.zeros_like(bound_pad)
    right_pad[...] = jnp.zeros_like(right_pad)
    left_dense[...] = jnp.zeros_like(left_dense)
    pl.semaphore_wait(barrier, 4)

    def z_copy():
        return pltpu.make_async_remote_copy(
            src_ref=right_hbm.at[0], dst_ref=right_all.at[me, cols - 1],
            send_sem=z_sem.at[0], recv_sem=z_sem.at[1],
            device_id={"col": col_left}, device_id_type=MESH,
        )

    def link(which, route, c):
        buffer = bound_all if which == 0 else right_all
        slot = across if route == 2 else me
        target = across if route == 0 else partner
        return pltpu.make_async_remote_copy(
            src_ref=buffer.at[slot, c], dst_ref=buffer.at[slot, c],
            send_sem=send_sem.at[which, route, c], recv_sem=recv_sem.at[which, route, c],
            device_id={"blk": target}, device_id_type=MESH,
        )

    z_copy().start()
    own_copies[0].wait()
    link(0, 0, 0).start()
    own_copies[1].wait()
    for c in range(cols):
        if c > 0:
            link(0, 0, c).start()
        if c < cols - 1:
            link(1, 0, c).start()
    for c in range(cols):
        link(0, 1, c).start()
        if c < cols - 1:
            link(1, 1, c).start()
    own_copies[2].wait()
    own_copies[3].wait()

    z_copy().wait_recv()
    link(1, 0, cols - 1).start()
    link(1, 1, cols - 1).start()

    def scalars(c):
        at = here * cols + c
        nxt = (at + 1) % all_cols
        p0 = [legs[0, k, at] for k in range(D)]
        p1 = [legs[1, k, at] for k in range(D)]
        p2 = [legs[2, k, at] for k in range(D)]
        pr = [legs[0, k, nxt] for k in range(D)]
        return p0, p1, p2, pr, charges[0, at], charges[1, at], charges[0, nxt], charges[1, nxt]

    lane96 = lax.broadcasted_iota(jnp.int32, (subs, BLOCK), 1)
    row96 = lax.broadcasted_iota(jnp.int32, (subs, BLOCK), 0)

    def as_mask(condition):
        return jnp.where(condition, 1.0, 0.0)

    def prepare(c, _):
        p0, p1, p2, pr, in_here, out_here, in_next, out_next = scalars(c)
        for l in range(D):
            q = (parity + p0[l]) % 2
            segment = left_own[c, :, l * BLOCK:(l + 1) * BLOCK]
            keep = lane96 < limit_of(in_here, q)
            even = as_mask(keep & (q == 0)).astype(jnp.bfloat16)
            odd = as_mask(keep & (q == 1)).astype(jnp.bfloat16)
            left_dense[c, l * subs:(l + 1) * subs, 0:BLOCK] = segment * even
            left_dense[c, l * subs:(l + 1) * subs, LANES:LANES + BLOCK] = segment * odd
        w = row_wide[pl.ds(c, D * D * D, stride=cols), :][:, 0:D].astype(jnp.bfloat16)
        spread_row = lax.broadcasted_iota(jnp.int32, (KRON, D), 0)
        spread_lane = lax.broadcasted_iota(jnp.int32, (KRON, D), 1)
        spread = as_mask((spread_row // SUB) % D == spread_lane).astype(jnp.bfloat16)
        big = lax.dot_general(
            spread, w, (((1,), (1,)), ((), ())), preferred_element_type=jnp.float32
        )
        row = lax.broadcasted_iota(jnp.int32, (KRON, KRON), 0)
        lane = lax.broadcasted_iota(jnp.int32, (KRON, KRON), 1)
        flat_row = lax.broadcasted_iota(jnp.int32, (KRON, D * D * D), 0)
        flat_lane = lax.broadcasted_iota(jnp.int32, (KRON, D * D * D), 1)
        big = jnp.where(flat_row // (D * SUB) == flat_lane % D, big, 0.0).astype(jnp.bfloat16)
        group_row = lax.broadcasted_iota(jnp.int32, (D * D * D, KRON), 0)
        group_lane = lax.broadcasted_iota(jnp.int32, (D * D * D, KRON), 1)
        group = as_mask(group_row // D == group_lane // SUB).astype(jnp.bfloat16)
        big = jnp.dot(big, group, preferred_element_type=jnp.float32)
        rows = lax.broadcasted_iota(jnp.int32, (KRON, 1), 0)
        lanes = lax.broadcasted_iota(jnp.int32, (1, KRON), 1)
        down = pick(rows // (D * SUB), p2)
        right = pick((rows // SUB) % D, pr)
        left = pick(lanes // (D * SUB), p0)
        up = pick((lanes // SUB) % D, p1)
        row_sign = 1 - 2 * (((parity + down + right) % 2) * down)
        lane_sign = 1 - 2 * left * up
        row_par = (down + right) % 2
        lane_par = (left + up) % 2
        same = row_par * lane_par + (1 - row_par) * (1 - lane_par)
        factor = (same * row_sign * lane_sign).astype(jnp.float32)
        kron[c] = jnp.where(row % SUB == lane % SUB, big * factor, 0.0).astype(jnp.bfloat16)
        return _

    row_wide[:, 0:D] = row_own[...].astype(jnp.float32)
    lax.fori_loop(0, cols, prepare, 0)

    def out_copy(c):
        return pltpu.make_async_copy(out_own.at[c], out_ref.at[c], out_sem.at[c])

    def column(c, _):
        p0, p1, p2, pr, in_here, out_here, in_next, out_next = scalars(c)
        link(1, 0, c).wait_recv()
        link(1, 2, c).start()
        link(0, 1, c).wait_recv()
        link(0, 2, c).wait_recv()
        for slot in range(n_blk):
            top = (slot // 2) * LANES + (slot % 2) * subs
            for u in range(D):
                bound_pad[top:top + subs, u * LANES:u * LANES + BLOCK] = bound_all[
                    slot, c, :, u * BLOCK:(u + 1) * BLOCK
                ]
        absorbed = jnp.dot(left_dense[c], bound_pad[...], preferred_element_type=jnp.float32)
        high = subs // SUB
        x = jnp.concatenate(
            [
                jnp.concatenate(
                    [
                        absorbed[l * subs + h * SUB:l * subs + (h + 1) * SUB, u * LANES:(u + 1) * LANES]
                        for h in range(high)
                    ],
                    axis=1,
                )
                for l in range(D)
                for u in range(D)
            ],
            axis=0,
        ).astype(jnp.bfloat16)
        mixed = jnp.dot(kron[c], x, preferred_element_type=jnp.float32)
        y_ref[...] = jnp.concatenate(
            [
                jnp.concatenate(
                    [
                        mixed[(d * D + r) * SUB:(d * D + r + 1) * SUB, h * LANES:(h + 1) * LANES]
                        for r in range(D)
                    ],
                    axis=1,
                )
                for d in range(D)
                for h in range(high)
            ],
            axis=0,
        ).astype(jnp.bfloat16)

        @pl.when(c + 1 < cols)
        def advance():
            link(0, 0, c + 1).wait_recv()
            link(0, 2, c + 1).start()

        link(1, 1, c).wait_recv()
        link(1, 2, c).wait_recv()
        for half in range(2):
            even_live = as_mask(row96 + half * subs < in_next).astype(jnp.bfloat16)
            odd_live = as_mask(row96 + half * subs < CHI - in_next).astype(jnp.bfloat16)
            for r in range(D):
                span = slice(r * BLOCK, (r + 1) * BLOCK)
                even = right_all[half, c, :, span] * even_live
                odd = right_all[2 + half, c, :, span] * odd_live
                straight = (parity + pr[r]) % 2 == 0
                top = r * LANES + half * subs
                right_pad[top:top + subs, 0:BLOCK] = jnp.where(straight, even, odd)
                right_pad[top:top + subs, LANES:LANES + BLOCK] = jnp.where(straight, odd, even)
        result = jnp.dot(y_ref[...], right_pad[...], preferred_element_type=jnp.float32)
        row_live = row96 + row_base < limit_of(out_here, parity)
        for d in range(D):
            rows = slice(d * subs, (d + 1) * subs)
            part = jnp.where(p2[d] == 0, result[rows, 0:BLOCK], result[rows, LANES:LANES + BLOCK])
            live = row_live & (lane96 < limit_of(out_next, (parity + p2[d]) % 2))
            out_own[c, :, d * BLOCK:(d + 1) * BLOCK] = jnp.where(live, part, 0.0).astype(jnp.bfloat16)
        out_copy(c).start()
        return _

    link(0, 0, 0).wait_recv()
    link(0, 2, 0).start()
    lax.fori_loop(0, cols, column, 0)

    z_copy().wait_send()
    for c in range(cols):
        out_copy(c).wait()
        for which in range(2):
            for route in range(3):
                link(which, route, c).wait_send()


def per_device(n_blk, n_col, boundary, row_tensor, left_proj, right_proj, leg_parity, bond_charges):
    cols, subs, merged = boundary.shape
    bf16 = jnp.bfloat16
    row_flat = row_tensor.transpose(1, 2, 3, 0, 4).reshape(D * D * D * cols, D)
    hbm = pl.BlockSpec(memory_space=pl.ANY)
    smem = pl.BlockSpec(memory_space=pltpu.SMEM)
    return pl.pallas_call(
        functools.partial(kernel, cols, subs, n_blk, n_col),
        out_shape=jax.ShapeDtypeStruct(boundary.shape, bf16),
        in_specs=[hbm, hbm, hbm, hbm, smem, smem],
        out_specs=hbm,
        scratch_shapes=[
            pltpu.VMEM((n_blk, cols, subs, merged), bf16),
            pltpu.VMEM((n_blk, cols, subs, merged), bf16),
            pltpu.VMEM((cols, subs, merged), bf16),
            pltpu.VMEM(row_flat.shape, bf16),
            pltpu.VMEM((row_flat.shape[0], LANES), jnp.float32),
            pltpu.VMEM((cols, D * subs, 2 * LANES), bf16),
            pltpu.VMEM((cols, KRON, KRON), bf16),
            pltpu.VMEM((2 * LANES, D * LANES), bf16),
            pltpu.VMEM((D * LANES, 2 * LANES), bf16),
            pltpu.VMEM((D * subs, D * LANES), bf16),
            pltpu.VMEM(boundary.shape, bf16),
            pltpu.SemaphoreType.DMA((4,)),
            pltpu.SemaphoreType.DMA((2, 3, cols)),
            pltpu.SemaphoreType.DMA((2, 3, cols)),
            pltpu.SemaphoreType.DMA((2,)),
            pltpu.SemaphoreType.DMA((cols,)),
        ],
        compiler_params=pltpu.CompilerParams(
            collective_id=0, has_side_effects=True
        ),
    )(boundary, row_flat, left_proj, right_proj, leg_parity.transpose(1, 2, 0), bond_charges.T)


def solution(mesh):
    in_specs = (
        P(("grp", "col"), "blk", None),
        P(("grp", "col"), None, None, None, None),
        P(("grp", "col"), "blk", None),
        P(("grp", "col"), "blk", None),
        P("grp", None, None),
        P("grp", None),
    )
    out_specs = P(("grp", "col"), "blk", None)
    body = functools.partial(per_device, mesh.shape["blk"], mesh.shape["col"])
    return jax.shard_map(body, mesh=mesh, in_specs=in_specs, out_specs=out_specs, check_vma=False)
```

```python
import functools

import jax
import jax.numpy as jnp
from jax import lax
from jax.experimental import pallas as pl
from jax.experimental.pallas import tpu as pltpu
from jax.sharding import PartitionSpec as P

CHI = 128
BLOCK = 96
D = 6
LANES = 128
SUB = 8
KRON = D * D * SUB
MESH = pl.DeviceIdType.MESH


def limit_of(count, parity):
    return jnp.where(parity == 0, count, CHI - count)


def pick(index, scalars):
    acc = jnp.zeros(index.shape, jnp.int32)
    for at, value in enumerate(scalars):
        acc = jnp.where(index == at, value, acc)
    return acc


def kernel(
    cols, subs, n_blk, n_col,
    bound_hbm, row_hbm, left_hbm, right_hbm, legs, charges, out_ref,
    bound_all, right_all, left_own, row_own, row_wide, left_dense, kron, bound_pad, right_pad, y_ref, out_own,
    local_sem, send_sem, recv_sem, z_sem, out_sem, group_in, col_in,
):
    me = lax.axis_index("blk")
    here = lax.axis_index("col")
    partner = me + 1 - 2 * (me % 2)
    across = (me + 2) % n_blk
    across_partner = (partner + 2) % n_blk
    col_left = (here + n_col - 1) % n_col
    col_right = (here + 1) % n_col
    all_cols = cols * n_col
    parity = me // 2
    row_base = (me % 2) * subs

    own_copies = [
        pltpu.make_async_copy(bound_hbm, bound_all.at[me], local_sem.at[0]),
        pltpu.make_async_copy(
            right_hbm.at[pl.ds(1, cols - 1)], right_all.at[me, pl.ds(0, cols - 1)], local_sem.at[1]
        ),
        pltpu.make_async_copy(left_hbm, left_own, local_sem.at[2]),
        pltpu.make_async_copy(row_hbm, row_own, local_sem.at[3]),
    ]
    for copy in own_copies:
        copy.start()

    barrier = pltpu.get_barrier_semaphore()

    @pl.when(me % 2 == 0)
    def hub_enters():
        pl.semaphore_signal(barrier, inc=1, device_id={"blk": across}, device_id_type=MESH)

    @pl.when(me % 2 == 1)
    def other_enters():
        pl.semaphore_signal(barrier, inc=1, device_id={"blk": partner}, device_id_type=MESH)
        pl.semaphore_signal(barrier, inc=1, device_id={"blk": across_partner}, device_id_type=MESH)

    bound_pad[...] = jnp.zeros_like(bound_pad)
    right_pad[...] = jnp.zeros_like(right_pad)
    left_dense[...] = jnp.zeros_like(left_dense)

    @pl.when(me % 2 == 0)
    def hub_knows():
        pl.semaphore_wait(barrier, n_blk - 1)
        pl.semaphore_signal(group_in, inc=1, device_id={"blk": partner}, device_id_type=MESH)

    @pl.when(me % 2 == 1)
    def other_knows():
        pl.semaphore_wait(group_in, 1)
        pl.semaphore_signal(barrier, inc=1, device_id={"col": col_right}, device_id_type=MESH)

    def z_copy():
        return pltpu.make_async_remote_copy(
            src_ref=right_hbm.at[0], dst_ref=right_all.at[me, cols - 1],
            send_sem=z_sem.at[0], recv_sem=z_sem.at[1],
            device_id={"col": col_left}, device_id_type=MESH,
        )

    def link(which, route, c):
        buffer = bound_all if which == 0 else right_all
        slot = across if route == 2 else me
        target = across if route == 0 else partner
        return pltpu.make_async_remote_copy(
            src_ref=buffer.at[slot, c], dst_ref=buffer.at[slot, c],
            send_sem=send_sem.at[which, route, c], recv_sem=recv_sem.at[which, route, c],
            device_id={"blk": target}, device_id_type=MESH,
        )

    own_copies[0].wait()
    link(0, 0, 0).start()
    own_copies[1].wait()
    for c in range(cols):
        if c > 0:
            link(0, 0, c).start()
        if c < cols - 1:
            link(1, 0, c).start()
    for c in range(cols):
        link(0, 1, c).start()
        if c < cols - 1:
            link(1, 1, c).start()
    own_copies[2].wait()
    own_copies[3].wait()

    def scalars(c):
        at = here * cols + c
        nxt = (at + 1) % all_cols
        p0 = [legs[0, k, at] for k in range(D)]
        p1 = [legs[1, k, at] for k in range(D)]
        p2 = [legs[2, k, at] for k in range(D)]
        pr = [legs[0, k, nxt] for k in range(D)]
        return p0, p1, p2, pr, charges[0, at], charges[1, at], charges[0, nxt], charges[1, nxt]

    lane96 = lax.broadcasted_iota(jnp.int32, (subs, BLOCK), 1)
    row96 = lax.broadcasted_iota(jnp.int32, (subs, BLOCK), 0)

    def as_mask(condition):
        return jnp.where(condition, 1.0, 0.0)

    def prepare(c, _):
        p0, p1, p2, pr, in_here, out_here, in_next, out_next = scalars(c)
        for l in range(D):
            q = (parity + p0[l]) % 2
            segment = left_own[c, :, l * BLOCK:(l + 1) * BLOCK]
            keep = lane96 < limit_of(in_here, q)
            even = as_mask(keep & (q == 0)).astype(jnp.bfloat16)
            odd = as_mask(keep & (q == 1)).astype(jnp.bfloat16)
            left_dense[c, l * subs:(l + 1) * subs, 0:BLOCK] = segment * even
            left_dense[c, l * subs:(l + 1) * subs, LANES:LANES + BLOCK] = segment * odd
        w = row_wide[pl.ds(c, D * D * D, stride=cols), :][:, 0:D].astype(jnp.bfloat16)
        spread_row = lax.broadcasted_iota(jnp.int32, (KRON, D), 0)
        spread_lane = lax.broadcasted_iota(jnp.int32, (KRON, D), 1)
        spread = as_mask((spread_row // SUB) % D == spread_lane).astype(jnp.bfloat16)
        big = lax.dot_general(
            spread, w, (((1,), (1,)), ((), ())), preferred_element_type=jnp.float32
        )
        row = lax.broadcasted_iota(jnp.int32, (KRON, KRON), 0)
        lane = lax.broadcasted_iota(jnp.int32, (KRON, KRON), 1)
        flat_row = lax.broadcasted_iota(jnp.int32, (KRON, D * D * D), 0)
        flat_lane = lax.broadcasted_iota(jnp.int32, (KRON, D * D * D), 1)
        big = jnp.where(flat_row // (D * SUB) == flat_lane % D, big, 0.0).astype(jnp.bfloat16)
        group_row = lax.broadcasted_iota(jnp.int32, (D * D * D, KRON), 0)
        group_lane = lax.broadcasted_iota(jnp.int32, (D * D * D, KRON), 1)
        group = as_mask(group_row // D == group_lane // SUB).astype(jnp.bfloat16)
        big = jnp.dot(big, group, preferred_element_type=jnp.float32)
        rows = lax.broadcasted_iota(jnp.int32, (KRON, 1), 0)
        lanes = lax.broadcasted_iota(jnp.int32, (1, KRON), 1)
        down = pick(rows // (D * SUB), p2)
        right = pick((rows // SUB) % D, pr)
        left = pick(lanes // (D * SUB), p0)
        up = pick((lanes // SUB) % D, p1)
        row_sign = 1 - 2 * (((parity + down + right) % 2) * down)
        lane_sign = 1 - 2 * left * up
        row_par = (down + right) % 2
        lane_par = (left + up) % 2
        same = row_par * lane_par + (1 - row_par) * (1 - lane_par)
        factor = (same * row_sign * lane_sign).astype(jnp.float32)
        kron[c] = jnp.where(row % SUB == lane % SUB, big * factor, 0.0).astype(jnp.bfloat16)
        return _

    row_wide[:, 0:D] = row_own[...].astype(jnp.float32)
    lax.fori_loop(0, cols // 2, prepare, 0)

    @pl.when(me % 2 == 1)
    def other_meets():
        pl.semaphore_wait(barrier, 1)
        pl.semaphore_signal(col_in, inc=1, device_id={"blk": partner}, device_id_type=MESH)

    @pl.when(me % 2 == 0)
    def hub_meets():
        pl.semaphore_wait(col_in, 1)

    z_copy().start()
    lax.fori_loop(cols // 2, cols, prepare, 0)

    def out_copy(c):
        return pltpu.make_async_copy(out_own.at[c], out_ref.at[c], out_sem.at[c])

    def column(c, _):
        p0, p1, p2, pr, in_here, out_here, in_next, out_next = scalars(c)
        link(1, 0, c).wait_recv()
        link(1, 2, c).start()
        link(0, 1, c).wait_recv()
        link(0, 2, c).wait_recv()
        for slot in range(n_blk):
            top = (slot // 2) * LANES + (slot % 2) * subs
            for u in range(D):
                bound_pad[top:top + subs, u * LANES:u * LANES + BLOCK] = bound_all[
                    slot, c, :, u * BLOCK:(u + 1) * BLOCK
                ]
        absorbed = jnp.dot(left_dense[c], bound_pad[...], preferred_element_type=jnp.float32)
        high = subs // SUB
        x = jnp.concatenate(
            [
                jnp.concatenate(
                    [
                        absorbed[l * subs + h * SUB:l * subs + (h + 1) * SUB, u * LANES:(u + 1) * LANES]
                        for h in range(high)
                    ],
                    axis=1,
                )
                for l in range(D)
                for u in range(D)
            ],
            axis=0,
        ).astype(jnp.bfloat16)
        mixed = jnp.dot(kron[c], x, preferred_element_type=jnp.float32)
        y_ref[...] = jnp.concatenate(
            [
                jnp.concatenate(
                    [
                        mixed[(d * D + r) * SUB:(d * D + r + 1) * SUB, h * LANES:(h + 1) * LANES]
                        for r in range(D)
                    ],
                    axis=1,
                )
                for d in range(D)
                for h in range(high)
            ],
            axis=0,
        ).astype(jnp.bfloat16)

        @pl.when(c == max(cols - 3, 0))
        def beyond():
            z_copy().wait_recv()
            link(1, 0, cols - 1).start()
            link(1, 1, cols - 1).start()

        @pl.when(c + 1 < cols)
        def advance():
            link(0, 0, c + 1).wait_recv()
            link(0, 2, c + 1).start()

        link(1, 1, c).wait_recv()
        link(1, 2, c).wait_recv()
        for half in range(2):
            even_live = as_mask(row96 + half * subs < in_next).astype(jnp.bfloat16)
            odd_live = as_mask(row96 + half * subs < CHI - in_next).astype(jnp.bfloat16)
            for r in range(D):
                span = slice(r * BLOCK, (r + 1) * BLOCK)
                even = right_all[half, c, :, span] * even_live
                odd = right_all[2 + half, c, :, span] * odd_live
                straight = (parity + pr[r]) % 2 == 0
                top = r * LANES + half * subs
                right_pad[top:top + subs, 0:BLOCK] = jnp.where(straight, even, odd)
                right_pad[top:top + subs, LANES:LANES + BLOCK] = jnp.where(straight, odd, even)
        result = jnp.dot(y_ref[...], right_pad[...], preferred_element_type=jnp.float32)
        row_live = row96 + row_base < limit_of(out_here, parity)
        for d in range(D):
            rows = slice(d * subs, (d + 1) * subs)
            part = jnp.where(p2[d] == 0, result[rows, 0:BLOCK], result[rows, LANES:LANES + BLOCK])
            live = row_live & (lane96 < limit_of(out_next, (parity + p2[d]) % 2))
            out_own[c, :, d * BLOCK:(d + 1) * BLOCK] = jnp.where(live, part, 0.0).astype(jnp.bfloat16)
        out_copy(c).start()
        return _

    link(0, 0, 0).wait_recv()
    link(0, 2, 0).start()
    lax.fori_loop(0, cols, column, 0)

    z_copy().wait_send()
    for c in range(cols):
        out_copy(c).wait()
        for which in range(2):
            for route in range(3):
                link(which, route, c).wait_send()


def per_device(n_blk, n_col, boundary, row_tensor, left_proj, right_proj, leg_parity, bond_charges):
    cols, subs, merged = boundary.shape
    bf16 = jnp.bfloat16
    row_flat = row_tensor.transpose(1, 2, 3, 0, 4).reshape(D * D * D * cols, D)
    hbm = pl.BlockSpec(memory_space=pl.ANY)
    smem = pl.BlockSpec(memory_space=pltpu.SMEM)
    return pl.pallas_call(
        functools.partial(kernel, cols, subs, n_blk, n_col),
        out_shape=jax.ShapeDtypeStruct(boundary.shape, bf16),
        in_specs=[hbm, hbm, hbm, hbm, smem, smem],
        out_specs=hbm,
        scratch_shapes=[
            pltpu.VMEM((n_blk, cols, subs, merged), bf16),
            pltpu.VMEM((n_blk, cols, subs, merged), bf16),
            pltpu.VMEM((cols, subs, merged), bf16),
            pltpu.VMEM(row_flat.shape, bf16),
            pltpu.VMEM((row_flat.shape[0], LANES), jnp.float32),
            pltpu.VMEM((cols, D * subs, 2 * LANES), bf16),
            pltpu.VMEM((cols, KRON, KRON), bf16),
            pltpu.VMEM((2 * LANES, D * LANES), bf16),
            pltpu.VMEM((D * LANES, 2 * LANES), bf16),
            pltpu.VMEM((D * subs, D * LANES), bf16),
            pltpu.VMEM(boundary.shape, bf16),
            pltpu.SemaphoreType.DMA((4,)),
            pltpu.SemaphoreType.DMA((2, 3, cols)),
            pltpu.SemaphoreType.DMA((2, 3, cols)),
            pltpu.SemaphoreType.DMA((2,)),
            pltpu.SemaphoreType.DMA((cols,)),
            pltpu.SemaphoreType.REGULAR,
            pltpu.SemaphoreType.REGULAR,
        ],
        compiler_params=pltpu.CompilerParams(
            collective_id=0, has_side_effects=True
        ),
    )(boundary, row_flat, left_proj, right_proj, leg_parity.transpose(1, 2, 0), bond_charges.T)


def solution(mesh):
    in_specs = (
        P(("grp", "col"), "blk", None),
        P(("grp", "col"), None, None, None, None),
        P(("grp", "col"), "blk", None),
        P(("grp", "col"), "blk", None),
        P("grp", None, None),
        P("grp", None),
    )
    out_specs = P(("grp", "col"), "blk", None)
    body = functools.partial(per_device, mesh.shape["blk"], mesh.shape["col"])
    return jax.shard_map(body, mesh=mesh, in_specs=in_specs, out_specs=out_specs, check_vma=False)
```

```python
import functools

import jax
import jax.numpy as jnp
from jax import lax
from jax.experimental import pallas as pl
from jax.experimental.pallas import tpu as pltpu
from jax.sharding import PartitionSpec as P

CHI = 128
BLOCK = 96
D = 6
LANES = 128
SUB = 8
KRON = D * D * SUB
MESH = pl.DeviceIdType.MESH


def limit_of(count, parity):
    return jnp.where(parity == 0, count, CHI - count)


def pick(index, scalars):
    acc = jnp.zeros(index.shape, jnp.int32)
    for at, value in enumerate(scalars):
        acc = jnp.where(index == at, value, acc)
    return acc


def kernel(
    cols, subs, n_blk, n_col,
    bound_hbm, row_hbm, left_hbm, right_hbm, legs_hbm, charges_hbm, out_ref,
    main_all, tail_all, bound_own, right_own, left_own, row_own, row_wide, left_dense, kron, bound_pad, right_pad, y_ref, out_own,
    legs, charges, local_sem, send_sem, recv_sem, z_sem, out_sem, group_in, col_in,
):
    me = lax.axis_index("blk")
    wide = D * BLOCK // LANES * LANES
    rest = D * BLOCK - wide
    here = lax.axis_index("col")
    partner = me + 1 - 2 * (me % 2)
    across = (me + 2) % n_blk
    across_partner = (partner + 2) % n_blk
    col_left = (here + n_col - 1) % n_col
    col_right = (here + 1) % n_col
    all_cols = cols * n_col
    parity = me // 2
    row_base = (me % 2) * subs

    own_copies = [
        pltpu.make_async_copy(bound_hbm, bound_own, local_sem.at[0]),
        pltpu.make_async_copy(
            right_hbm.at[pl.ds(1, cols - 1)], right_own.at[pl.ds(0, cols - 1)], local_sem.at[1]
        ),
        pltpu.make_async_copy(left_hbm, left_own, local_sem.at[2]),
        pltpu.make_async_copy(row_hbm, row_own, local_sem.at[3]),
        pltpu.make_async_copy(
            bound_hbm.at[:, :, pl.ds(0, wide)], main_all.at[0, me], local_sem.at[4]
        ),
        pltpu.make_async_copy(
            right_hbm.at[pl.ds(1, cols - 1), :, pl.ds(0, wide)],
            main_all.at[1, me, pl.ds(0, cols - 1)], local_sem.at[5]
        ),
        pltpu.make_async_copy(legs_hbm, legs, local_sem.at[6]),
        pltpu.make_async_copy(charges_hbm, charges, local_sem.at[7]),
    ]
    for k in (4, 5, 0, 1, 2, 3, 6, 7):
        own_copies[k].start()

    barrier = pltpu.get_barrier_semaphore()

    @pl.when(me % 2 == 0)
    def hub_enters():
        pl.semaphore_signal(barrier, inc=1, device_id={"blk": across}, device_id_type=MESH)

    @pl.when(me % 2 == 1)
    def other_enters():
        pl.semaphore_signal(barrier, inc=1, device_id={"blk": partner}, device_id_type=MESH)
        pl.semaphore_signal(barrier, inc=1, device_id={"blk": across_partner}, device_id_type=MESH)

    bound_pad[...] = jnp.zeros_like(bound_pad)
    right_pad[...] = jnp.zeros_like(right_pad)
    left_dense[...] = jnp.zeros_like(left_dense)

    @pl.when(me % 2 == 0)
    def hub_knows():
        pl.semaphore_wait(barrier, n_blk - 1)
        pl.semaphore_signal(group_in, inc=1, device_id={"blk": partner}, device_id_type=MESH)

    @pl.when(me % 2 == 1)
    def other_knows():
        pl.semaphore_wait(group_in, 1)
        pl.semaphore_signal(barrier, inc=1, device_id={"col": col_right}, device_id_type=MESH)

    def z_copy():
        return pltpu.make_async_remote_copy(
            src_ref=right_hbm.at[0], dst_ref=right_own.at[cols - 1],
            send_sem=z_sem.at[0], recv_sem=z_sem.at[1],
            device_id={"col": col_left}, device_id_type=MESH,
        )

    def link(which, route, c):
        slot = across if route == 2 else me
        target = across if route == 0 else partner
        piece = tail_all.at[slot, c] if which == 2 else main_all.at[which, slot, c]
        return pltpu.make_async_remote_copy(
            src_ref=piece, dst_ref=piece,
            send_sem=send_sem.at[which, route, c], recv_sem=recv_sem.at[which, route, c],
            device_id={"blk": target}, device_id_type=MESH,
        )

    own_copies[4].wait()
    link(0, 0, 0).start()
    own_copies[5].wait()
    link(1, 0, 0).start()
    for c in range(cols):
        link(0, 1, c).start()
        if c < cols - 1:
            link(1, 1, c).start()
    own_copies[0].wait()
    own_copies[1].wait()
    for c in range(cols - 1):
        tail_all[me, c] = jnp.concatenate([bound_own[c, :, wide:], right_own[c, :, wide:]], axis=1)
    for c in range(cols):
        if c > 0:
            link(0, 0, c).start()
        if c < cols - 1:
            link(2, 0, c).start()
            link(2, 1, c).start()
            if c > 0:
                link(1, 0, c).start()
    own_copies[2].wait()
    own_copies[3].wait()
    own_copies[6].wait()
    own_copies[7].wait()

    def scalars(c):
        at = here * cols + c
        nxt = (at + 1) % all_cols
        p0 = [legs[0, k, at] for k in range(D)]
        p1 = [legs[1, k, at] for k in range(D)]
        p2 = [legs[2, k, at] for k in range(D)]
        pr = [legs[0, k, nxt] for k in range(D)]
        return p0, p1, p2, pr, charges[0, at], charges[1, at], charges[0, nxt], charges[1, nxt]

    lane96 = lax.broadcasted_iota(jnp.int32, (subs, BLOCK), 1)
    row96 = lax.broadcasted_iota(jnp.int32, (subs, BLOCK), 0)

    def as_mask(condition):
        return jnp.where(condition, 1.0, 0.0)

    def prepare(c, _):
        p0, p1, p2, pr, in_here, out_here, in_next, out_next = scalars(c)
        for l in range(D):
            q = (parity + p0[l]) % 2
            segment = left_own[c, :, l * BLOCK:(l + 1) * BLOCK]
            keep = lane96 < limit_of(in_here, q)
            even = as_mask(keep & (q == 0)).astype(jnp.bfloat16)
            odd = as_mask(keep & (q == 1)).astype(jnp.bfloat16)
            left_dense[c, l * subs:(l + 1) * subs, 0:BLOCK] = segment * even
            left_dense[c, l * subs:(l + 1) * subs, LANES:LANES + BLOCK] = segment * odd
        w = row_wide[pl.ds(c, D * D * D, stride=cols), :][:, 0:D].astype(jnp.bfloat16)
        spread_row = lax.broadcasted_iota(jnp.int32, (KRON, D), 0)
        spread_lane = lax.broadcasted_iota(jnp.int32, (KRON, D), 1)
        spread = as_mask((spread_row // SUB) % D == spread_lane).astype(jnp.bfloat16)
        big = lax.dot_general(
            spread, w, (((1,), (1,)), ((), ())), preferred_element_type=jnp.float32
        )
        row = lax.broadcasted_iota(jnp.int32, (KRON, KRON), 0)
        lane = lax.broadcasted_iota(jnp.int32, (KRON, KRON), 1)
        flat_row = lax.broadcasted_iota(jnp.int32, (KRON, D * D * D), 0)
        flat_lane = lax.broadcasted_iota(jnp.int32, (KRON, D * D * D), 1)
        big = jnp.where(flat_row // (D * SUB) == flat_lane % D, big, 0.0).astype(jnp.bfloat16)
        group_row = lax.broadcasted_iota(jnp.int32, (D * D * D, KRON), 0)
        group_lane = lax.broadcasted_iota(jnp.int32, (D * D * D, KRON), 1)
        group = as_mask(group_row // D == group_lane // SUB).astype(jnp.bfloat16)
        big = jnp.dot(big, group, preferred_element_type=jnp.float32)
        rows = lax.broadcasted_iota(jnp.int32, (KRON, 1), 0)
        lanes = lax.broadcasted_iota(jnp.int32, (1, KRON), 1)
        down = pick(rows // (D * SUB), p2)
        right = pick((rows // SUB) % D, pr)
        left = pick(lanes // (D * SUB), p0)
        up = pick((lanes // SUB) % D, p1)
        row_sign = 1 - 2 * (((parity + down + right) % 2) * down)
        lane_sign = 1 - 2 * left * up
        row_par = (down + right) % 2
        lane_par = (left + up) % 2
        same = row_par * lane_par + (1 - row_par) * (1 - lane_par)
        factor = (same * row_sign * lane_sign).astype(jnp.float32)
        kron[c] = jnp.where(row % SUB == lane % SUB, big * factor, 0.0).astype(jnp.bfloat16)
        return _

    row_wide[:, 0:D] = row_own[...].astype(jnp.float32)
    lax.fori_loop(0, cols // 2, prepare, 0)

    @pl.when(me % 2 == 1)
    def other_meets():
        pl.semaphore_wait(barrier, 1)
        pl.semaphore_signal(col_in, inc=1, device_id={"blk": partner}, device_id_type=MESH)

    @pl.when(me % 2 == 0)
    def hub_meets():
        pl.semaphore_wait(col_in, 1)

    z_copy().start()
    lax.fori_loop(cols // 2, cols, prepare, 0)

    def segment_of(which, slot, c, leg):
        low = leg * BLOCK
        if low + BLOCK <= wide:
            return main_all[which, slot, c, :, low:low + BLOCK]
        return jnp.concatenate(
            [main_all[which, slot, c, :, low:wide], tail_all[slot, c, :, which * rest:(which + 1) * rest]],
            axis=1,
        )

    def out_copy(c):
        return pltpu.make_async_copy(out_own.at[c], out_ref.at[c], out_sem.at[c])

    def column(c, _):
        p0, p1, p2, pr, in_here, out_here, in_next, out_next = scalars(c)
        link(1, 0, c).wait_recv()
        link(1, 2, c).start()
        for which in (0, 2):
            link(which, 1, c).wait_recv()
            link(which, 2, c).wait_recv()
        for slot in range(n_blk):
            top = (slot // 2) * LANES + (slot % 2) * subs
            for u in range(D):
                bound_pad[top:top + subs, u * LANES:u * LANES + BLOCK] = segment_of(0, slot, c, u)
        absorbed = jnp.dot(left_dense[c], bound_pad[...], preferred_element_type=jnp.float32)
        high = subs // SUB
        x = jnp.concatenate(
            [
                jnp.concatenate(
                    [
                        absorbed[l * subs + h * SUB:l * subs + (h + 1) * SUB, u * LANES:(u + 1) * LANES]
                        for h in range(high)
                    ],
                    axis=1,
                )
                for l in range(D)
                for u in range(D)
            ],
            axis=0,
        ).astype(jnp.bfloat16)
        mixed = jnp.dot(kron[c], x, preferred_element_type=jnp.float32)
        y_ref[...] = jnp.concatenate(
            [
                jnp.concatenate(
                    [
                        mixed[(d * D + r) * SUB:(d * D + r + 1) * SUB, h * LANES:(h + 1) * LANES]
                        for r in range(D)
                    ],
                    axis=1,
                )
                for d in range(D)
                for h in range(high)
            ],
            axis=0,
        ).astype(jnp.bfloat16)

        @pl.when(c == 0)
        def beyond():
            z_copy().wait_recv()
            main_all[1, me, cols - 1] = right_own[cols - 1, :, 0:wide]
            tail_all[me, cols - 1] = jnp.concatenate(
                [bound_own[cols - 1, :, wide:], right_own[cols - 1, :, wide:]], axis=1
            )
            for route in range(2):
                link(2, route, cols - 1).start()
                link(1, route, cols - 1).start()

        @pl.when(c + 1 < cols)
        def advance():
            for which in (0, 2):
                link(which, 0, c + 1).wait_recv()
                link(which, 2, c + 1).start()

        link(1, 1, c).wait_recv()
        link(1, 2, c).wait_recv()
        for half in range(2):
            even_live = as_mask(row96 + half * subs < in_next).astype(jnp.bfloat16)
            odd_live = as_mask(row96 + half * subs < CHI - in_next).astype(jnp.bfloat16)
            for r in range(D):
                even = segment_of(1, half, c, r) * even_live
                odd = segment_of(1, 2 + half, c, r) * odd_live
                straight = (parity + pr[r]) % 2 == 0
                top = r * LANES + half * subs
                right_pad[top:top + subs, 0:BLOCK] = jnp.where(straight, even, odd)
                right_pad[top:top + subs, LANES:LANES + BLOCK] = jnp.where(straight, odd, even)
        result = jnp.dot(y_ref[...], right_pad[...], preferred_element_type=jnp.float32)
        row_live = row96 + row_base < limit_of(out_here, parity)
        for d in range(D):
            rows = slice(d * subs, (d + 1) * subs)
            part = jnp.where(p2[d] == 0, result[rows, 0:BLOCK], result[rows, LANES:LANES + BLOCK])
            live = row_live & (lane96 < limit_of(out_next, (parity + p2[d]) % 2))
            out_own[c, :, d * BLOCK:(d + 1) * BLOCK] = jnp.where(live, part, 0.0).astype(jnp.bfloat16)
        out_copy(c).start()
        return _

    for which in (0, 2):
        link(which, 0, 0).wait_recv()
        link(which, 2, 0).start()
    lax.fori_loop(0, cols, column, 0)

    z_copy().wait_send()
    for c in range(cols):
        out_copy(c).wait()
        for which in range(3):
            for route in range(3):
                link(which, route, c).wait_send()


def per_device(n_blk, n_col, boundary, row_tensor, left_proj, right_proj, leg_parity, bond_charges):
    cols, subs, merged = boundary.shape
    bf16 = jnp.bfloat16
    row_flat = row_tensor.transpose(1, 2, 3, 0, 4).reshape(D * D * D * cols, D)
    hbm = pl.BlockSpec(memory_space=pl.ANY)
    return pl.pallas_call(
        functools.partial(kernel, cols, subs, n_blk, n_col),
        out_shape=jax.ShapeDtypeStruct(boundary.shape, bf16),
        in_specs=[hbm] * 6,
        out_specs=hbm,
        scratch_shapes=[
            pltpu.VMEM((2, n_blk, cols, subs, merged // LANES * LANES), bf16),
            pltpu.VMEM((n_blk, cols, subs, LANES), bf16),
            pltpu.VMEM((cols, subs, merged), bf16),
            pltpu.VMEM((cols, subs, merged), bf16),
            pltpu.VMEM((cols, subs, merged), bf16),
            pltpu.VMEM(row_flat.shape, bf16),
            pltpu.VMEM((row_flat.shape[0], LANES), jnp.float32),
            pltpu.VMEM((cols, D * subs, 2 * LANES), bf16),
            pltpu.VMEM((cols, KRON, KRON), bf16),
            pltpu.VMEM((2 * LANES, D * LANES), bf16),
            pltpu.VMEM((D * LANES, 2 * LANES), bf16),
            pltpu.VMEM((D * subs, D * LANES), bf16),
            pltpu.VMEM(boundary.shape, bf16),
            pltpu.SMEM(leg_parity.shape[1:] + leg_parity.shape[:1], jnp.int32),
            pltpu.SMEM(bond_charges.shape[::-1], jnp.int32),
            pltpu.SemaphoreType.DMA((8,)),
            pltpu.SemaphoreType.DMA((3, 3, cols)),
            pltpu.SemaphoreType.DMA((3, 3, cols)),
            pltpu.SemaphoreType.DMA((2,)),
            pltpu.SemaphoreType.DMA((cols,)),
            pltpu.SemaphoreType.REGULAR,
            pltpu.SemaphoreType.REGULAR,
        ],
        compiler_params=pltpu.CompilerParams(
            collective_id=0, has_side_effects=True
        ),
    )(boundary, row_flat, left_proj, right_proj, leg_parity.transpose(1, 2, 0), bond_charges.T)


def solution(mesh):
    in_specs = (
        P(("grp", "col"), "blk", None),
        P(("grp", "col"), None, None, None, None),
        P(("grp", "col"), "blk", None),
        P(("grp", "col"), "blk", None),
        P("grp", None, None),
        P("grp", None),
    )
    out_specs = P(("grp", "col"), "blk", None)
    body = functools.partial(per_device, mesh.shape["blk"], mesh.shape["col"])
    return jax.shard_map(body, mesh=mesh, in_specs=in_specs, out_specs=out_specs, check_vma=False)
```
